256 devices in a mesh: groups: 2 (over z), owners: 16 (over x, core), sub: 8 (over y).
Axes of the slice: x: 8, y: 8, z: 2, core: 2. Of those that a mesh axis runs over, the one named last changes fastest.
The devices are a block of a 8x8x16 slice.
Arguments:
- embeddings: bfloat16 [131072, 768], P(('groups', 'owners', 'sub')), parts along dimension 0, may hold values from -6 to 6, as said below
- class_table: bfloat16 [1000, 768], replicated, may hold values from -6 to 6
- nearest: int32 [131072], P(('groups', 'owners', 'sub')), parts along dimension 0, may hold values from 0 to 999
- keep_class: int32 [1000], replicated, may hold values 0 or 1
- destination: int32 [131072, 1], P(('groups', 'owners', 'sub')), parts along dimension 0, may hold values from 0 to 127; in each aligned block of 512 rows (0 to 511, 512 to 1023, ...) at most 6 rows name the same one
Outputs:
- received_rows: bfloat16 [196608, 768], P(('groups', 'owners', 'sub')), parts along dimension 0
- received_score: bfloat16 [196608], P(('groups', 'owners', 'sub')), parts along dimension 0
- received_position: int32 [196608], P(('groups', 'owners', 'sub')), parts along dimension 0
- shard_totals: int32 [256], P('groups'), parts along dimension 0
The draws below stay inside these ranges and needn't reach their ends.
There are 2 independent parts, one for each index of `groups`. The reference program is written for one: setup_inputs(seed, part) draws one part's arguments, and reference() takes and returns one part's arrays. A program takes and returns all parts, laid end to end along the dimension named above; an argument that names none is the same for every part. Nothing has to cross between parts.
Inputs may be any that keep to these rules, and one draw needn't show every extreme that they name: `destination`: in the rows of one device no loader shard is named by more than 6 rows. Counts of rows per loader shard may be packed several to an int32 word wherever they travel; this is an exception to the 16-bit rule below. `embeddings`: some rows are entirely zero.
All inputs are finite; a program needn't handle non-finite values.
Results may differ from the reference program's by a relative error of at most 0.001.
Values may be sent and summed in bfloat16 or wider, within the bound.
A program may use at most 64 MiB of HBM per device.

```python
import math
import jax
import jax.numpy as jnp
import numpy as np
from jax import lax

D = 768
CLASSES = 1000
ROWS_DEV = 512
NDEST = 128
CAP = 6
ROWS = 65536


def draw_embeddings(key, part):
    value_key = jax.random.fold_in(key, 11)
    blank_key = jax.random.fold_in(key, 13)
    values = jnp.clip(jax.random.normal(value_key, (ROWS, D), jnp.float32), -6.0, 6.0)
    blank = jax.random.randint(blank_key, (ROWS, 1), 0, 64) == 0
    values = jnp.where(blank, jnp.float32(0.0), values)
    return values.astype(jnp.bfloat16)


def plant(values, own_key, least, high):
    dims = values.shape
    spot = [jax.random.randint(jax.random.fold_in(own_key, axis), (), 0, dims[axis]) for axis in range(len(dims))]
    values = values.at[tuple(spot)].set(least)
    longest = dims.index(max(dims))
    spot[longest] = (spot[longest] + 1) % dims[longest]
    return values.at[tuple(spot)].set(high)


def routed_block(rng, own, number, rows, count, top, bound, slope):
    ranking = jax.random.permutation(rng, count)
    heavy_load, ordinary = shares(count, rows * top, bound, slope, True), shares(count, rows * top, bound, slope, False)
    places = jnp.arange(count)

    def named(tallies, turn):
        used = int((tallies > 0).sum())
        fixed = max(1, used // 4)
        passed = fixed + (places - fixed + turn * (used - fixed)) % max(1, count - fixed)
        return jnp.zeros((count,), jnp.int32).at[ranking[jnp.where(places < fixed, places, passed)]].set(jnp.asarray(tallies, jnp.int32))

    tallies = jnp.where(number % 4 == 0, named(heavy_load, number // 4), named(ordinary, number - number // 4 - 1))
    mixed = jax.random.permutation(jax.random.fold_in(own, 3), count)
    donor, taker = mixed[0:count // 2 * 2:2], mixed[1:count // 2 * 2:2]
    slack = jnp.minimum(tallies[donor] - 1, bound - tallies[taker]) // 2
    slack = jnp.where((donor == ranking[0]) | (taker == ranking[0]) | (tallies[taker] == 0), 0, jnp.maximum(slack, 0))
    passed = jax.random.randint(jax.random.fold_in(own, 4), (count // 2,), 0, 1 << 20) % (slack + 1)
    tallies = tallies.at[donor].add(-passed).at[taker].add(passed)
    items = jnp.searchsorted(jnp.cumsum(tallies), jnp.arange(rows * top), side="right").astype(jnp.int32)
    table = items.reshape(top, rows).T
    table = table[jax.random.permutation(jax.random.fold_in(own, 1), rows)]
    turn = jax.random.randint(jax.random.fold_in(own, 2), (rows, 1), 0, top)
    return jnp.take_along_axis(table, (jnp.arange(top)[None, :] + turn) % top, axis=1)


def shares(amount, total, bound, lean, full):
    portions = [(1 << 20) // math.isqrt(rank ** lean) + 1 for rank in range(1, amount + 1)]
    largest = bound if full else min(bound, max(-(-total // amount), total * portions[0] // sum(portions)))
    least = 1 if total - largest >= amount - 1 else 0
    holding, rest = [largest] + [least] * (amount - 1), total - largest - least * (amount - 1)
    while rest > 0:
        candidates = [i for i in range(1, amount) if holding[i] < largest] or [i for i in range(1, amount) if holding[i] < bound]
        mass, budget = sum([portions[i] for i in candidates]), rest
        for i in candidates:
            more = min(bound - holding[i], max(1, budget * portions[i] // mass), rest)
            holding[i] = holding[i] + more
            rest = rest - more
    return np.array(holding)


def noise(stream_key, extent, scale, most, kind=jnp.bfloat16):
    return jnp.clip(scale * jax.random.normal(stream_key, extent, jnp.float32), -most, most).astype(kind)


def setup_inputs(seed: int = 0, part: int = 0) -> dict:
    keys = jax.random.split(jax.random.key(seed), 6)
    own_keys = jax.random.split(jax.random.fold_in(keys[5], part), 6)
    embeddings = draw_embeddings(jax.random.fold_in(jax.random.fold_in(keys[5], part), 71), part)
    class_table = noise(keys[1], (CLASSES, D), 1.0, 6.0)
    nearest = plant(jax.random.randint(own_keys[2], (ROWS,), 0, CLASSES), jax.random.fold_in(own_keys[2], 1), 0, CLASSES - 1).astype(jnp.int32)
    keep_class = plant((jax.random.randint(keys[3], (CLASSES,), 0, 4) < 3).astype(jnp.int32), jax.random.fold_in(keys[3], 1), 0, 1)
    destination_keys = jax.random.split(jax.random.fold_in(own_keys[4], 1), ROWS // ROWS_DEV)
    destination_turns = jax.random.permutation(jax.random.fold_in(own_keys[4], 3), ROWS // ROWS_DEV)
    destination = jax.vmap(lambda own, number: routed_block(jax.random.fold_in(own_keys[4], 2), own, number, ROWS_DEV, NDEST, 1, CAP, 2))(destination_keys, destination_turns).reshape((ROWS, 1))
    return dict(embeddings=embeddings, class_table=class_table, nearest=nearest, keep_class=keep_class, destination=destination)


def margins(row_block, near_block, class_table, inverse_class, keep_class):
    products = jnp.dot(row_block, class_table.T, preferred_element_type=jnp.float32)
    squares = row_block.astype(jnp.float32) * row_block.astype(jnp.float32)
    inverse_row = lax.rsqrt(lax.optimization_barrier(jnp.sum(squares, axis=1)) + 1e-06)
    cosine = products * inverse_row[:, None] * inverse_class[None, :]
    class_ids = jnp.arange(class_table.shape[0], dtype=jnp.int32)
    class_match = near_block[:, None] == class_ids[None, :]
    given_cos = lax.optimization_barrier(jnp.sum(jnp.where(class_match, cosine, 0.0), axis=1))
    others = lax.optimization_barrier(jnp.max(jnp.where(class_match, -1e+30, cosine), axis=1))
    kept_flag = lax.optimization_barrier(jnp.sum(jnp.where(class_match, keep_class[None, :], 0), axis=1)).astype(jnp.int32)
    return (20.0 * (given_cos - others), kept_flag)

def reference(embeddings, class_table, nearest, keep_class, destination):
    class_float = class_table.astype(jnp.float32)
    inverse_class = lax.rsqrt(lax.optimization_barrier(jnp.sum(class_float * class_float, axis=1)) + 1e-06)
    total_rows = embeddings.shape[0]
    block_rows = math.gcd(total_rows, 1024)

    def one_block(inputs):
        return margins(inputs[0], inputs[1], class_table, inverse_class, keep_class)
    margin_value, kept_flag = lax.map(one_block, (embeddings.reshape(total_rows // block_rows, block_rows, D), nearest.reshape(total_rows // block_rows, block_rows)))
    margin_value = margin_value.reshape(total_rows)
    kept_flag = kept_flag.reshape(total_rows)
    target = destination[:, 0].astype(jnp.int32)
    shard_ids = jnp.arange(NDEST, dtype=jnp.int32)
    onehot = ((target[:, None] == shard_ids[None, :]) & (kept_flag[:, None] == 1)).astype(jnp.int32)
    running = jnp.cumsum(onehot, axis=0) - onehot
    global_rank = jnp.take_along_axis(running, target[:, None], axis=1)[:, 0].astype(jnp.int32)
    block_start = running.reshape(NDEST, ROWS_DEV, NDEST)[:, 0, :]
    source = (jnp.arange(total_rows, dtype=jnp.int32) // ROWS_DEV).astype(jnp.int32)
    local_rank = (global_rank - block_start[source, target]).astype(jnp.int32)
    slot_count = NDEST * NDEST * CAP
    slot_index = jnp.where(kept_flag == 1, (target * NDEST + source) * CAP + local_rank, slot_count).astype(jnp.int32)
    received_rows = jnp.zeros((slot_count, D), jnp.bfloat16).at[slot_index].set(embeddings, mode='drop')
    received_score = jnp.zeros((slot_count,), jnp.bfloat16).at[slot_index].set(margin_value.astype(jnp.bfloat16), mode='drop')
    received_position = jnp.full((slot_count,), -1, jnp.int32).at[slot_index].set(global_rank, mode='drop')
    shard_totals = lax.optimization_barrier(jnp.sum(onehot, axis=0)).astype(jnp.int32)
    return (received_rows, received_score, received_position, shard_totals)
```

```python
import functools

import jax
import jax.numpy as jnp
from jax import lax
from jax.experimental import pallas as pl
from jax.experimental.pallas import tpu as pltpu
from jax.sharding import PartitionSpec as P

MESH = pl.DeviceIdType.MESH
BF = jnp.bfloat16
F32 = jnp.float32
ROWS_AXES = ("groups", "owners", "sub")


def iota(shape, dim):
    return lax.broadcasted_iota(jnp.int32, shape, dim)


def as_bf(mask):
    return jnp.where(mask, 1.0, 0.0).astype(BF)


def dot(a, b, dims):
    return lax.dot_general(a, b, (dims, ((), ())), preferred_element_type=F32)


def peer_of(step, own, sub, n_own, n_sub):
    shift = lax.rem(step * 37, n_own * n_sub)
    by_own, by_sub = shift // n_sub, lax.rem(shift, n_sub)
    chip = lax.rem(own // 2 + by_own // 2, n_own // 2)
    core = lax.rem(own + by_own, 2)
    return chip * 2 + core, lax.rem(sub + by_sub, n_sub)


def kernel(
    n_own, n_sub, cap,
    emb_hbm, table_hbm, near_hbm, keep_hbm, dest_hbm,
    rows_out, pos_out, score_out, total_out,
    emb, table, near, keep, dest, sbuf, smeta, rmeta,
    load_sem, own_sem, row_send, row_recv, meta_send, meta_recv,
):
    own, sub = lax.axis_index("owners"), lax.axis_index("sub")
    n = n_own * n_sub
    me = own * n_sub + sub
    rows, depth = emb.shape
    classes = table.shape[0]

    barrier = pltpu.get_barrier_semaphore()

    def greet(step, carry):
        o, s = peer_of(step, own, sub, n_own, n_sub)
        pl.semaphore_signal(
            barrier, inc=1, device_id={"owners": o, "sub": s}, device_id_type=MESH
        )
        return carry

    loads = [
        pltpu.make_async_copy(src, dst, load_sem.at[i])
        for i, (src, dst) in enumerate(
            (
                (near_hbm, near),
                (keep_hbm, keep),
                (dest_hbm, dest),
                (emb_hbm, emb),
                (table_hbm, table),
            )
        )
    ]
    for load in loads:
        load.start()
    lax.fori_loop(1, n, greet, 0)

    loads[0].wait()
    loads[1].wait()
    loads[2].wait()
    near_v = near[...]
    matches = near_v == iota((classes, rows), 0)
    kept = dot(keep[...].astype(F32).astype(BF), as_bf(matches), ((1,), (0,)))
    named = (dest[...] == iota((n, rows), 0)) & (kept > 0.5)
    named_bf = as_bf(named)
    earlier = as_bf(iota((rows, rows), 0) < iota((rows, rows), 1))
    running = dot(named_bf, earlier, ((1,), (0,)))
    rank = jnp.sum(jnp.where(named, running, 0.0), axis=0, keepdims=True).astype(jnp.int32)
    slot = jnp.where(kept > 0.5, dest[...] * cap + rank, -1)
    place = as_bf(slot == iota((n * cap, rows), 0))
    counts = dot(jnp.ones((8, rows), BF), named_bf, ((1,), (1,)))[:1]

    loads[3].wait()
    packed = dot(place, emb[...], ((1,), (0,))).astype(BF)
    sbuf[...] = packed.reshape(n, cap // 2, 2, depth)

    pl.semaphore_wait(barrier, n - 1)

    def send_rows(step, carry):
        o, s = peer_of(step, own, sub, n_own, n_sub)
        pltpu.make_async_remote_copy(
            sbuf.at[o * n_sub + s], rows_out.at[me], row_send, row_recv,
            device_id={"owners": o, "sub": s}, device_id_type=MESH,
        ).start()
        return carry

    lax.fori_loop(1, n, send_rows, 0)
    own_copy = pltpu.make_async_copy(sbuf.at[me], rows_out.at[me], own_sem)
    own_copy.start()

    loads[4].wait()
    emb_f = emb[...].astype(F32)
    row_square = jnp.sum(emb_f * emb_f, axis=1, keepdims=True)
    inv_row = lax.rsqrt(jnp.transpose(jnp.broadcast_to(row_square, (rows, 128)))[:1] + 1e-6)
    table_f = table[...].astype(F32)
    inv_class = lax.rsqrt(jnp.sum(table_f * table_f, axis=1, keepdims=True) + 1e-6)
    cosine = dot(table[...], emb[...], ((1,), (1,))) * inv_class
    given = jnp.sum(jnp.where(matches, cosine, 0.0), axis=0, keepdims=True)
    others = jnp.max(jnp.where(matches, -1e30, cosine), axis=0, keepdims=True)
    margin = (20.0 * ((given - others) * inv_row)).astype(BF).astype(F32)
    by_rank = jnp.where(rank == iota((8, rows), 0), margin, 0.0).astype(BF)
    scores = dot(named_bf, by_rank, ((1,), (1,)))
    scores = jnp.concatenate([scores, jnp.zeros((n, 120), F32)], axis=1)
    meta = jnp.stack([jnp.broadcast_to(counts, (n, n)), scores], axis=1)
    smeta[...] = meta.astype(BF)
    rmeta[me] = smeta[me]

    def send_meta(step, carry):
        o, s = peer_of(step, own, sub, n_own, n_sub)
        pltpu.make_async_remote_copy(
            smeta.at[o * n_sub + s], rmeta.at[me], meta_send, meta_recv,
            device_id={"owners": o, "sub": s}, device_id_type=MESH,
        ).start()
        return carry

    lax.fori_loop(1, n, send_meta, 0)
    part = pl.ds(0, n - 1)
    pltpu.make_async_copy(smeta.at[part], rmeta.at[part], meta_recv).wait()

    got = rmeta[...].astype(F32)
    got_counts, got_scores = got[:, 0, :], got[:, 1, :]
    slots = n * cap
    source = iota((n, slots), 1) // cap
    step_in = lax.rem(iota((1, slots), 1), cap)
    spread = as_bf(iota((n, slots), 0) == source)
    before = as_bf(iota((n, slots), 0) < source)
    counts_bf = got_counts.astype(BF)
    mine = iota((n, slots), 0) == me
    filled = jnp.sum(jnp.where(mine, dot(counts_bf, spread, ((0,), (0,))), 0.0), axis=0, keepdims=True)
    base = jnp.sum(jnp.where(mine, dot(counts_bf, before, ((0,), (0,))), 0.0), axis=0, keepdims=True)
    pos_out[...] = jnp.where(
        step_in < filled.astype(jnp.int32), base.astype(jnp.int32) + step_in, -1
    )
    spread_scores = dot(got_scores[:, :8].astype(BF), spread, ((0,), (0,)))
    score_out[...] = jnp.sum(
        jnp.where(iota((8, slots), 0) == step_in, spread_scores, 0.0), axis=0, keepdims=True
    ).astype(BF)
    total_out[...] = jnp.sum(got_counts, axis=0, keepdims=True).astype(jnp.int32)

    pltpu.make_async_copy(smeta.at[part], rmeta.at[part], meta_send).wait()
    pltpu.make_async_copy(sbuf.at[part], rows_out.at[part], row_send).wait()
    own_copy.wait()
    pltpu.make_async_copy(sbuf.at[part], rows_out.at[part], row_recv).wait()


def on_device(n_own, n_sub, embeddings, class_table, nearest, keep_class, destination):
    rows, depth = embeddings.shape
    classes = class_table.shape[0]
    n = n_own * n_sub
    cap = 3 * rows // (2 * n)
    slots = n * cap
    vmem = pl.BlockSpec(memory_space=pltpu.VMEM)
    hbm = pl.BlockSpec(memory_space=pl.ANY)
    got_rows, position, score, totals = pl.pallas_call(
        functools.partial(kernel, n_own, n_sub, cap),
        out_shape=(
            jax.ShapeDtypeStruct((n, cap // 2, 2, depth), BF),
            jax.ShapeDtypeStruct((1, slots), jnp.int32),
            jax.ShapeDtypeStruct((1, slots), BF),
            jax.ShapeDtypeStruct((1, n), jnp.int32),
        ),
        in_specs=[hbm] * 5,
        out_specs=(hbm, vmem, vmem, vmem),
        scratch_shapes=[
            pltpu.VMEM((rows, depth), BF),
            pltpu.VMEM((classes, depth), BF),
            pltpu.VMEM((1, rows), jnp.int32),
            pltpu.VMEM((1, classes), jnp.int32),
            pltpu.VMEM((1, rows), jnp.int32),
            pltpu.VMEM((n, cap // 2, 2, depth), BF),
            pltpu.VMEM((n, 2, 128), BF),
            pltpu.VMEM((n, 2, 128), BF),
            pltpu.SemaphoreType.DMA((5,)),
        ]
        + [pltpu.SemaphoreType.DMA] * 5,
        compiler_params=pltpu.CompilerParams(collective_id=0, has_side_effects=True),
    )(
        embeddings,
        class_table,
        nearest.reshape(1, rows),
        keep_class.reshape(1, classes),
        destination.reshape(1, rows),
    )
    return (
        got_rows.reshape(slots, depth),
        score.reshape(slots),
        position.reshape(slots),
        totals.reshape(n),
    )


def solution(mesh):
    spec = P(ROWS_AXES)
    return jax.shard_map(
        functools.partial(on_device, mesh.shape["owners"], mesh.shape["sub"]),
        mesh=mesh,
        in_specs=(P(ROWS_AXES, None), P(), spec, P(), P(ROWS_AXES, None)),
        out_specs=(P(ROWS_AXES, None), spec, spec, P("groups")),
        check_vma=False,
    )
```

```python
import functools

import jax
import jax.numpy as jnp
from jax import lax
from jax.experimental import pallas as pl
from jax.experimental.pallas import tpu as pltpu
from jax.sharding import PartitionSpec as P

MESH = pl.DeviceIdType.MESH
BF = jnp.bfloat16
F32 = jnp.float32
ROWS_AXES = ("groups", "owners", "sub")


def iota(shape, dim):
    return lax.broadcasted_iota(jnp.int32, shape, dim)


def as_bf(mask):
    return jnp.where(mask, 1.0, 0.0).astype(BF)


def dot(a, b, dims):
    return lax.dot_general(a, b, (dims, ((), ())), preferred_element_type=F32)


def turned(own, step, n_own):
    chip = lax.rem(own // 2 + step // 2, n_own // 2)
    return chip * 2 + lax.rem(own + step, 2)


def exchange(
    n_own, n_sub, cap,
    emb_hbm, table_hbm, near_hbm, keep_hbm, dest_hbm,
    got_rows, got_meta,
    emb, table, near, keep, dest, sbuf, smeta,
    load_sem, own_sem, row_send, row_recv, meta_send, meta_recv, in_sem, late_sem,
):
    own, sub = lax.axis_index("owners"), lax.axis_index("sub")
    n = n_own * n_sub
    me = own * n_sub + sub
    rows, depth = emb.shape
    classes = table.shape[0]

    barrier = pltpu.get_barrier_semaphore()
    late = me == 0
    early = jnp.logical_not(late)

    def tell(sem, o, s):
        pl.semaphore_signal(
            sem, inc=1, device_id={"owners": o, "sub": s}, device_id_type=MESH
        )

    loads = [
        pltpu.make_async_copy(src, dst, load_sem.at[i])
        for i, (src, dst) in enumerate(
            (
                (near_hbm, near),
                (keep_hbm, keep),
                (dest_hbm, dest),
                (emb_hbm, emb),
                (table_hbm, table),
            )
        )
    ]
    for load in loads:
        load.start()

    def greet_row(step, carry):
        o = turned(own, step, n_own)

        @pl.when(early & (o * n_sub + sub != 0))
        def _():
            tell(barrier, o, sub)

        return carry

    lax.fori_loop(1, n_own, greet_row, 0)

    loads[0].wait()
    loads[1].wait()
    loads[2].wait()
    near_v = near[...]
    matches = near_v == iota((classes, rows), 0)
    kept = dot(keep[...].astype(F32).astype(BF), as_bf(matches), ((1,), (0,)))
    named = (dest[...] == iota((n, rows), 0)) & (kept > 0.5)
    named_bf = as_bf(named)
    earlier = as_bf(iota((rows, rows), 0) < iota((rows, rows), 1))
    running = dot(named_bf, earlier, ((1,), (0,)))
    rank = jnp.sum(jnp.where(named, running, 0.0), axis=0, keepdims=True).astype(jnp.int32)
    slot = jnp.where(kept > 0.5, dest[...] * cap + rank, -1)
    place = as_bf(slot == iota((n * cap, rows), 0))
    counts = dot(jnp.ones((8, rows), BF), named_bf, ((1,), (1,)))[:1]

    loads[3].wait()
    packed = dot(place, emb[...], ((1,), (0,))).astype(BF)
    sbuf[...] = packed.reshape(n, cap // 2, 2, depth)

    @pl.when(early & (sub == 0))
    def _():
        pl.semaphore_wait(barrier, n_own - 2)
        tell(barrier, 0, 0)

    @pl.when(sub != 0)
    def _():
        pl.semaphore_wait(barrier, n_own - 1 + sub)

    @pl.when((own == 0) & (sub != 0))
    def _():
        tell(barrier, 0, 0)

    @pl.when(late)
    def _():
        pl.semaphore_wait(barrier, n_own - 1 + n_sub - 1)

    def tell_column(s, carry):
        @pl.when(early & (s > sub))
        def _():
            tell(barrier, own, s)

        @pl.when((own == 1) & (sub == 0) & (s > 0))
        def _():
            tell(barrier, 0, s)

        @pl.when((s < sub) & (own * n_sub + s != 0))
        def _():
            tell(in_sem.at[sub], own, s)

        return carry

    lax.fori_loop(0, n_sub, tell_column, 0)

    def tell_late(i, carry):
        @pl.when(late)
        def _():
            tell(late_sem, i // n_sub, lax.rem(i, n_sub))

        return carry

    lax.fori_loop(1, n, tell_late, 0)

    def send_rows(o, s):
        pltpu.make_async_remote_copy(
            sbuf.at[o * n_sub + s], got_rows.at[me], row_send, row_recv,
            device_id={"owners": o, "sub": s}, device_id_type=MESH,
        ).start()

    def send_meta(o, s):
        pltpu.make_async_remote_copy(
            smeta.at[o * n_sub + s], got_meta.at[me], meta_send, meta_recv,
            device_id={"owners": o, "sub": s}, device_id_type=MESH,
        ).start()

    def near_peers(act):
        def one(step, carry):
            shift = lax.rem(step * 37, n)
            o = turned(own, shift // n_sub, n_own)
            s = lax.rem(sub + shift, n_sub)

            @pl.when((late | (s <= sub)) & (o * n_sub + s != 0))
            def _():
                act(o, s)

            return carry

        lax.fori_loop(1, n, one, 0)

    near_peers(send_rows)
    own_rows = pltpu.make_async_copy(sbuf.at[me], got_rows.at[me], own_sem.at[0])
    own_rows.start()

    loads[4].wait()
    emb_f = emb[...].astype(F32)
    row_square = jnp.sum(emb_f * emb_f, axis=1, keepdims=True)
    inv_row = lax.rsqrt(jnp.transpose(jnp.broadcast_to(row_square, (rows, 128)))[:1] + 1e-6)
    table_f = table[...].astype(F32)
    inv_class = lax.rsqrt(jnp.sum(table_f * table_f, axis=1, keepdims=True) + 1e-6)
    cosine = dot(table[...], emb[...], ((1,), (1,))) * inv_class
    given = jnp.sum(jnp.where(matches, cosine, 0.0), axis=0, keepdims=True)
    rival = jnp.max(jnp.where(matches, -1e30, cosine), axis=0, keepdims=True)
    margin = (20.0 * ((given - rival) * inv_row)).astype(BF).astype(F32)
    by_rank = jnp.where(rank == iota((8, rows), 0), margin, 0.0).astype(BF)
    scores = dot(named_bf, by_rank, ((1,), (1,)))
    scores = jnp.concatenate([scores, jnp.zeros((n, 120), F32)], axis=1)
    meta = jnp.stack([jnp.broadcast_to(counts, (n, n)), scores], axis=1)
    smeta[...] = meta.astype(BF)

    near_peers(send_meta)
    own_meta = pltpu.make_async_copy(smeta.at[me], got_meta.at[me], own_sem.at[1])
    own_meta.start()

    for s in range(1, n_sub):

        @pl.when(early & (s > sub))
        def _():
            pl.semaphore_wait(in_sem.at[s], 1)

            def one(step, carry):
                o = turned(own, lax.rem(step * 5, n_own), n_own)
                send_rows(o, s)
                send_meta(o, s)
                return carry

            lax.fori_loop(0, n_own, one, 0)

    @pl.when(early)
    def _():
        pl.semaphore_wait(late_sem, 1)
        send_rows(0, 0)
        send_meta(0, 0)

    part = pl.ds(0, n - 1)
    pltpu.make_async_copy(sbuf.at[part], got_rows.at[part], row_send).wait()
    pltpu.make_async_copy(smeta.at[part], got_meta.at[part], meta_send).wait()
    own_rows.wait()
    own_meta.wait()
    pltpu.make_async_copy(sbuf.at[part], got_rows.at[part], row_recv).wait()
    pltpu.make_async_copy(smeta.at[part], got_meta.at[part], meta_recv).wait()


def finish(
    n_own, n_sub, cap,
    got_rows, got_meta,
    rows_out, score_out, pos_out, total_out,
    raw, meta, tidy, in_sem, out_sem, meta_sem,
):
    n = n_own * n_sub
    me = lax.axis_index("owners") * n_sub + lax.axis_index("sub")
    slots = n * cap
    depth = raw.shape[-1]
    load_meta = pltpu.make_async_copy(got_meta, meta, meta_sem)
    load_meta.start()
    loads, stores = [], []
    for g in range(n_own):
        block = pl.ds(g * n_sub, n_sub)
        span = pl.ds(g * n_sub * cap, n_sub * cap)
        loads.append(pltpu.make_async_copy(got_rows.at[block], raw.at[block], in_sem.at[g]))
        stores.append(pltpu.make_async_copy(tidy.at[span], rows_out.at[span], out_sem.at[g]))
        loads[-1].start()
    load_meta.wait()
    got = meta[...].astype(F32)
    got_counts, got_scores = got[:, 0, :], got[:, 1, :]
    source = iota((n, slots), 1) // cap
    step_in = lax.rem(iota((1, slots), 1), cap)
    spread = as_bf(iota((n, slots), 0) == source)
    before = as_bf(iota((n, slots), 0) < source)
    counts_bf = got_counts.astype(BF)
    mine = iota((n, slots), 0) == me
    filled = jnp.sum(
        jnp.where(mine, dot(counts_bf, spread, ((0,), (0,))), 0.0), axis=0, keepdims=True
    )
    base = jnp.sum(
        jnp.where(mine, dot(counts_bf, before, ((0,), (0,))), 0.0), axis=0, keepdims=True
    )
    pos_out[...] = jnp.where(
        step_in < filled.astype(jnp.int32), base.astype(jnp.int32) + step_in, -1
    ).reshape(slots)
    spread_scores = dot(got_scores[:, :8].astype(BF), spread, ((0,), (0,)))
    score_out[...] = (
        jnp.sum(
            jnp.where(iota((8, slots), 0) == step_in, spread_scores, 0.0), axis=0, keepdims=True
        )
        .astype(BF)
        .reshape(slots)
    )
    total_out[...] = jnp.sum(got_counts, axis=0, keepdims=True).astype(jnp.int32).reshape(n)
    for g in range(n_own):
        loads[g].wait()
        tidy[pl.ds(g * n_sub * cap, n_sub * cap), :] = raw[
            pl.ds(g * n_sub, n_sub)
        ].reshape(n_sub * cap, depth)
        stores[g].start()
    for store in stores:
        store.wait()


def on_device(n_own, n_sub, embeddings, class_table, nearest, keep_class, destination):
    rows, depth = embeddings.shape
    classes = class_table.shape[0]
    n = n_own * n_sub
    cap = 3 * rows // (2 * n)
    slots = n * cap
    vmem = pl.BlockSpec(memory_space=pltpu.VMEM)
    hbm = pl.BlockSpec(memory_space=pl.ANY)
    got_rows, got_meta = pl.pallas_call(
        functools.partial(exchange, n_own, n_sub, cap),
        out_shape=(
            jax.ShapeDtypeStruct((n, cap // 2, 2, depth), BF),
            jax.ShapeDtypeStruct((n, 2, 128), BF),
        ),
        in_specs=[hbm] * 5,
        out_specs=(hbm, hbm),
        scratch_shapes=[
            pltpu.VMEM((rows, depth), BF),
            pltpu.VMEM((classes, depth), BF),
            pltpu.VMEM((1, rows), jnp.int32),
            pltpu.VMEM((1, classes), jnp.int32),
            pltpu.VMEM((1, rows), jnp.int32),
            pltpu.VMEM((n, cap // 2, 2, depth), BF),
            pltpu.VMEM((n, 2, 128), BF),
            pltpu.SemaphoreType.DMA((5,)),
            pltpu.SemaphoreType.DMA((2,)),
            pltpu.SemaphoreType.DMA,
            pltpu.SemaphoreType.DMA,
            pltpu.SemaphoreType.DMA,
            pltpu.SemaphoreType.DMA,
            pltpu.SemaphoreType.REGULAR((n_sub,)),
            pltpu.SemaphoreType.REGULAR,
        ],
        compiler_params=pltpu.CompilerParams(collective_id=0, has_side_effects=True),
    )(
        embeddings,
        class_table,
        nearest.reshape(1, rows),
        keep_class.reshape(1, classes),
        destination.reshape(1, rows),
    )
    return pl.pallas_call(
        functools.partial(finish, n_own, n_sub, cap),
        out_shape=(
            jax.ShapeDtypeStruct((slots, depth), BF),
            jax.ShapeDtypeStruct((slots,), BF),
            jax.ShapeDtypeStruct((slots,), jnp.int32),
            jax.ShapeDtypeStruct((n,), jnp.int32),
        ),
        in_specs=[hbm, hbm],
        out_specs=(hbm, vmem, vmem, vmem),
        scratch_shapes=[
            pltpu.VMEM((n, cap // 2, 2, depth), BF),
            pltpu.VMEM((n, 2, 128), BF),
            pltpu.VMEM((slots, depth), BF),
            pltpu.SemaphoreType.DMA((n_own,)),
            pltpu.SemaphoreType.DMA((n_own,)),
            pltpu.SemaphoreType.DMA,
        ],
    )(got_rows, got_meta)


def solution(mesh):
    spec = P(ROWS_AXES)
    return jax.shard_map(
        functools.partial(on_device, mesh.shape["owners"], mesh.shape["sub"]),
        mesh=mesh,
        in_specs=(P(ROWS_AXES, None), P(), spec, P(), P(ROWS_AXES, None)),
        out_specs=(P(ROWS_AXES, None), spec, spec, P("groups")),
        check_vma=False,
    )
```

```python
import functools

import jax
import jax.numpy as jnp
from jax import lax
from jax.experimental import pallas as pl
from jax.experimental.pallas import tpu as pltpu
from jax.sharding import PartitionSpec as P

MESH = pl.DeviceIdType.MESH
BF = jnp.bfloat16
F32 = jnp.float32
ROWS_AXES = ("groups", "owners", "sub")


def iota(shape, dim):
    return lax.broadcasted_iota(jnp.int32, shape, dim)


def as_bf(mask):
    return jnp.where(mask, 1.0, 0.0).astype(BF)


def dot(a, b, dims):
    return lax.dot_general(a, b, (dims, ((), ())), preferred_element_type=F32)


def turned(own, step, n_own):
    chip = lax.rem(own // 2 + step // 2, n_own // 2)
    return chip * 2 + lax.rem(own + step, 2)


def exchange(
    n_own, n_sub, cap,
    emb_hbm, table_hbm, near_hbm, keep_hbm, dest_hbm,
    got_rows, got_meta,
    emb, table, near, keep, dest, sbuf, smeta,
    load_sem, own_sem, row_send, row_recv, meta_send, meta_recv, in_sem, late_sem,
):
    own, sub = lax.axis_index("owners"), lax.axis_index("sub")
    n = n_own * n_sub
    me = own * n_sub + sub
    rows, depth = emb.shape
    classes = table.shape[0]

    barrier = pltpu.get_barrier_semaphore()
    late = me == 0
    hold = n * 5 // 8
    early = jnp.logical_not(late)

    def tell(sem, o, s):
        pl.semaphore_signal(
            sem, inc=1, device_id={"owners": o, "sub": s}, device_id_type=MESH
        )

    loads = [
        pltpu.make_async_copy(src, dst, load_sem.at[i])
        for i, (src, dst) in enumerate(
            (
                (near_hbm, near),
                (keep_hbm, keep),
                (dest_hbm, dest),
                (emb_hbm, emb),
                (table_hbm, table),
            )
        )
    ]
    for load in loads:
        load.start()

    def greet_row(step, carry):
        o = turned(own, step, n_own)

        @pl.when(early & (o * n_sub + sub != 0))
        def _():
            tell(barrier, o, sub)

        return carry

    lax.fori_loop(1, n_own, greet_row, 0)

    loads[0].wait()
    loads[1].wait()
    loads[2].wait()
    near_v = near[...]
    matches = near_v == iota((classes, rows), 0)
    kept = dot(keep[...].astype(F32).astype(BF), as_bf(matches), ((1,), (0,)))
    named = (dest[...] == iota((n, rows), 0)) & (kept > 0.5)
    named_bf = as_bf(named)
    earlier = as_bf(iota((rows, rows), 0) < iota((rows, rows), 1))
    running = dot(named_bf, earlier, ((1,), (0,)))
    rank = jnp.sum(jnp.where(named, running, 0.0), axis=0, keepdims=True).astype(jnp.int32)
    slot = jnp.where(kept > 0.5, dest[...] * cap + rank, -1)
    place = as_bf(slot == iota((n * cap, rows), 0))
    counts = dot(jnp.ones((8, rows), BF), named_bf, ((1,), (1,)))[:1]

    loads[3].wait()
    packed = dot(place, emb[...], ((1,), (0,))).astype(BF)
    sbuf[...] = packed.reshape(n, cap // 2, 2, depth)

    @pl.when(early & (sub == 0))
    def _():
        pl.semaphore_wait(barrier, n_own - 2)
        tell(barrier, 0, 0)

    @pl.when(sub != 0)
    def _():
        pl.semaphore_wait(barrier, n_own - 1 + sub)

    @pl.when((own == 0) & (sub != 0))
    def _():
        tell(barrier, 0, 0)

    @pl.when(late)
    def _():
        pl.semaphore_wait(barrier, n_own - 1 + n_sub - 1)

    def tell_column(s, carry):
        @pl.when(early & (s > sub))
        def _():
            tell(barrier, own, s)

        @pl.when((own == 1) & (sub == 0) & (s > 0))
        def _():
            tell(barrier, 0, s)

        @pl.when((s < sub) & (own * n_sub + s != 0))
        def _():
            tell(in_sem.at[sub], own, s)

        return carry

    lax.fori_loop(0, n_sub, tell_column, 0)

    def tell_late(i, carry):
        @pl.when(late)
        def _():
            tell(late_sem, i // n_sub, lax.rem(i, n_sub))

        return carry

    lax.fori_loop(1, n, tell_late, 0)

    def send_rows(o, s):
        pltpu.make_async_remote_copy(
            sbuf.at[o * n_sub + s], got_rows.at[me], row_send, row_recv,
            device_id={"owners": o, "sub": s}, device_id_type=MESH,
        ).start()

    def send_meta(o, s):
        pltpu.make_async_remote_copy(
            smeta.at[o * n_sub + s], got_meta.at[me], meta_send, meta_recv,
            device_id={"owners": o, "sub": s}, device_id_type=MESH,
        ).start()

    def peers(act, first, last, which):
        def one(step, carry):
            shift = lax.rem(step * 37, n)
            o = turned(own, shift // n_sub, n_own)
            s = lax.rem(sub + shift, n_sub)

            @pl.when(which(s) & (o * n_sub + s != 0))
            def _():
                act(o, s)

            return carry

        lax.fori_loop(first, last, one, 0)

    peers(send_rows, 1, hold, lambda s: late | (s <= sub))
    own_rows = pltpu.make_async_copy(sbuf.at[me], got_rows.at[me], own_sem.at[0])
    own_rows.start()

    loads[4].wait()
    emb_f = emb[...].astype(F32)
    row_square = jnp.sum(emb_f * emb_f, axis=1, keepdims=True)
    inv_row = lax.rsqrt(jnp.transpose(jnp.broadcast_to(row_square, (rows, 128)))[:1] + 1e-6)
    table_f = table[...].astype(F32)
    inv_class = lax.rsqrt(jnp.sum(table_f * table_f, axis=1, keepdims=True) + 1e-6)
    cosine = dot(table[...], emb[...], ((1,), (1,))) * inv_class
    given = jnp.sum(jnp.where(matches, cosine, 0.0), axis=0, keepdims=True)
    rival = jnp.max(jnp.where(matches, -1e30, cosine), axis=0, keepdims=True)
    margin = (20.0 * ((given - rival) * inv_row)).astype(BF).astype(F32)
    by_rank = jnp.where(rank == iota((8, rows), 0), margin, 0.0).astype(BF)
    scores = dot(named_bf, by_rank, ((1,), (1,)))
    scores = jnp.concatenate([scores, jnp.zeros((n, 120), F32)], axis=1)
    meta = jnp.stack([jnp.broadcast_to(counts, (n, n)), scores], axis=1)
    smeta[...] = meta.astype(BF)

    own_meta = pltpu.make_async_copy(smeta.at[me], got_meta.at[me], own_sem.at[1])
    own_meta.start()

    for s in range(1, n_sub):

        @pl.when(early & (s > sub))
        def _():
            pl.semaphore_wait(in_sem.at[s], 1)

    peers(send_rows, 1, hold, lambda s: early & (s > sub))

    @pl.when(early)
    def _():
        pl.semaphore_wait(late_sem, 1)

    turn = hold + lax.rem(me, n - hold)

    def held(step, carry):
        @pl.when(early & (step == turn))
        def _():
            send_rows(0, 0)

        shift = lax.rem(step * 37, n)
        o = turned(own, shift // n_sub, n_own)
        s = lax.rem(sub + shift, n_sub)

        @pl.when(o * n_sub + s != 0)
        def _():
            send_rows(o, s)

        return carry

    lax.fori_loop(hold, n, held, 0)
    peers(send_meta, 1, n, lambda s: s >= 0)

    @pl.when(early)
    def _():
        send_meta(0, 0)

    part = pl.ds(0, n - 1)
    pltpu.make_async_copy(sbuf.at[part], got_rows.at[part], row_send).wait()
    pltpu.make_async_copy(smeta.at[part], got_meta.at[part], meta_send).wait()
    own_rows.wait()
    own_meta.wait()
    pltpu.make_async_copy(sbuf.at[part], got_rows.at[part], row_recv).wait()
    pltpu.make_async_copy(smeta.at[part], got_meta.at[part], meta_recv).wait()


def finish(
    n_own, n_sub, cap,
    got_rows, got_meta,
    rows_out, score_out, pos_out, total_out,
    raw, meta, tidy, in_sem, out_sem, meta_sem,
):
    n = n_own * n_sub
    me = lax.axis_index("owners") * n_sub + lax.axis_index("sub")
    slots = n * cap
    depth = raw.shape[-1]
    load_meta = pltpu.make_async_copy(got_meta, meta, meta_sem)
    load_meta.start()
    loads, stores = [], []
    for g in range(n_own):
        block = pl.ds(g * n_sub, n_sub)
        span = pl.ds(g * n_sub * cap, n_sub * cap)
        loads.append(pltpu.make_async_copy(got_rows.at[block], raw.at[block], in_sem.at[g]))
        stores.append(pltpu.make_async_copy(tidy.at[span], rows_out.at[span], out_sem.at[g]))
        loads[-1].start()
    for g in range(n_own):
        loads[g].wait()
        tidy[pl.ds(g * n_sub * cap, n_sub * cap), :] = raw[
            pl.ds(g * n_sub, n_sub)
        ].reshape(n_sub * cap, depth)
        stores[g].start()
    load_meta.wait()
    got = meta[...].astype(F32)
    got_counts, got_scores = got[:, 0, :], got[:, 1, :]
    source = iota((n, slots), 1) // cap
    step_in = lax.rem(iota((1, slots), 1), cap)
    spread = as_bf(iota((n, slots), 0) == source)
    before = as_bf(iota((n, slots), 0) < source)
    counts_bf = got_counts.astype(BF)
    mine = iota((n, slots), 0) == me
    filled = jnp.sum(
        jnp.where(mine, dot(counts_bf, spread, ((0,), (0,))), 0.0), axis=0, keepdims=True
    )
    base = jnp.sum(
        jnp.where(mine, dot(counts_bf, before, ((0,), (0,))), 0.0), axis=0, keepdims=True
    )
    pos_out[...] = jnp.where(
        step_in < filled.astype(jnp.int32), base.astype(jnp.int32) + step_in, -1
    ).reshape(slots)
    spread_scores = dot(got_scores[:, :8].astype(BF), spread, ((0,), (0,)))
    score_out[...] = (
        jnp.sum(
            jnp.where(iota((8, slots), 0) == step_in, spread_scores, 0.0), axis=0, keepdims=True
        )
        .astype(BF)
        .reshape(slots)
    )
    total_out[...] = jnp.sum(got_counts, axis=0, keepdims=True).astype(jnp.int32).reshape(n)
    for store in stores:
        store.wait()


def on_device(n_own, n_sub, embeddings, class_table, nearest, keep_class, destination):
    rows, depth = embeddings.shape
    classes = class_table.shape[0]
    n = n_own * n_sub
    cap = 3 * rows // (2 * n)
    slots = n * cap
    vmem = pl.BlockSpec(memory_space=pltpu.VMEM)
    hbm = pl.BlockSpec(memory_space=pl.ANY)
    got_rows, got_meta = pl.pallas_call(
        functools.partial(exchange, n_own, n_sub, cap),
        out_shape=(
            jax.ShapeDtypeStruct((n, cap // 2, 2, depth), BF),
            jax.ShapeDtypeStruct((n, 2, 128), BF),
        ),
        in_specs=[hbm] * 5,
        out_specs=(hbm, hbm),
        scratch_shapes=[
            pltpu.VMEM((rows, depth), BF),
            pltpu.VMEM((classes, depth), BF),
            pltpu.VMEM((1, rows), jnp.int32),
            pltpu.VMEM((1, classes), jnp.int32),
            pltpu.VMEM((1, rows), jnp.int32),
            pltpu.VMEM((n, cap // 2, 2, depth), BF),
            pltpu.VMEM((n, 2, 128), BF),
            pltpu.SemaphoreType.DMA((5,)),
            pltpu.SemaphoreType.DMA((2,)),
            pltpu.SemaphoreType.DMA,
            pltpu.SemaphoreType.DMA,
            pltpu.SemaphoreType.DMA,
            pltpu.SemaphoreType.DMA,
            pltpu.SemaphoreType.REGULAR((n_sub,)),
            pltpu.SemaphoreType.REGULAR,
        ],
        compiler_params=pltpu.CompilerParams(collective_id=0, has_side_effects=True),
    )(
        embeddings,
        class_table,
        nearest.reshape(1, rows),
        keep_class.reshape(1, classes),
        destination.reshape(1, rows),
    )
    return pl.pallas_call(
        functools.partial(finish, n_own, n_sub, cap),
        out_shape=(
            jax.ShapeDtypeStruct((slots, depth), BF),
            jax.ShapeDtypeStruct((slots,), BF),
            jax.ShapeDtypeStruct((slots,), jnp.int32),
            jax.ShapeDtypeStruct((n,), jnp.int32),
        ),
        in_specs=[hbm, hbm],
        out_specs=(hbm, vmem, vmem, vmem),
        scratch_shapes=[
            pltpu.VMEM((n, cap // 2, 2, depth), BF),
            pltpu.VMEM((n, 2, 128), BF),
            pltpu.VMEM((slots, depth), BF),
            pltpu.SemaphoreType.DMA((n_own,)),
            pltpu.SemaphoreType.DMA((n_own,)),
            pltpu.SemaphoreType.DMA,
        ],
    )(got_rows, got_meta)


def solution(mesh):
    spec = P(ROWS_AXES)
    return jax.shard_map(
        functools.partial(on_device, mesh.shape["owners"], mesh.shape["sub"]),
        mesh=mesh,
        in_specs=(P(ROWS_AXES, None), P(), spec, P(), P(ROWS_AXES, None)),
        out_specs=(P(ROWS_AXES, None), spec, spec, P("groups")),
        check_vma=False,
    )
```

```python
import functools

import jax
import jax.numpy as jnp
from jax import lax
from jax.experimental import pallas as pl
from jax.experimental.pallas import tpu as pltpu
from jax.sharding import PartitionSpec as P

MESH = pl.DeviceIdType.MESH
BF = jnp.bfloat16
F32 = jnp.float32
MIDDLE = 1
ROWS_AXES = ("groups", "owners", "sub")


def iota(shape, dim):
    return lax.broadcasted_iota(jnp.int32, shape, dim)


def as_bf(mask):
    return jnp.where(mask, 1.0, 0.0).astype(BF)


def dot(a, b, dims):
    return lax.dot_general(a, b, (dims, ((), ())), preferred_element_type=F32)


def turned(own, step, n_own):
    chip = lax.rem(own // 2 + step // 2, n_own // 2)
    return chip * 2 + lax.rem(own + step, 2)


def exchange(
    n_own, n_sub, cap,
    emb_hbm, table_hbm, near_hbm, keep_hbm, dest_hbm,
    got_rows, got_meta,
    emb, table, near, keep, dest, sbuf, smeta,
    load_sem, own_sem, row_send, row_recv, meta_send, meta_recv, in_sem, late_sem,
):
    own, sub = lax.axis_index("owners"), lax.axis_index("sub")
    n = n_own * n_sub
    me = own * n_sub + sub
    rows, depth = emb.shape
    classes = table.shape[0]

    barrier = pltpu.get_barrier_semaphore()
    late = me == 0
    hold = n * 5 // 8
    early = jnp.logical_not(late)

    def tell(sem, o, s):
        pl.semaphore_signal(
            sem, inc=1, device_id={"owners": o, "sub": s}, device_id_type=MESH
        )

    loads = [
        pltpu.make_async_copy(src, dst, load_sem.at[i])
        for i, (src, dst) in enumerate(
            (
                (near_hbm, near),
                (keep_hbm, keep),
                (dest_hbm, dest),
                (emb_hbm, emb),
                (table_hbm, table),
            )
        )
    ]
    for load in loads:
        load.start()

    def greet_row(step, carry):
        o = turned(own, step, n_own)

        @pl.when(early & (o * n_sub + sub != 0))
        def _():
            tell(barrier, o, sub)

        return carry

    lax.fori_loop(1, n_own, greet_row, 0)

    loads[0].wait()
    loads[1].wait()
    loads[2].wait()
    near_v = near[...]
    matches = near_v == iota((classes, rows), 0)
    kept = dot(keep[...].astype(F32).astype(BF), as_bf(matches), ((1,), (0,)))
    named = (dest[...] == iota((n, rows), 0)) & (kept > 0.5)
    named_bf = as_bf(named)
    earlier = as_bf(iota((rows, rows), 0) < iota((rows, rows), 1))
    running = dot(named_bf, earlier, ((1,), (0,)))
    rank = jnp.sum(jnp.where(named, running, 0.0), axis=0, keepdims=True).astype(jnp.int32)
    slot = jnp.where(kept > 0.5, dest[...] * cap + rank, -1)
    place = as_bf(slot == iota((n * cap, rows), 0))
    counts = dot(jnp.ones((8, rows), BF), named_bf, ((1,), (1,)))[:1]

    loads[3].wait()
    packed = dot(place, emb[...], ((1,), (0,))).astype(BF)
    sbuf[...] = packed.reshape(n, cap // 2, 2, depth)

    @pl.when(early & (sub == 0))
    def _():
        pl.semaphore_wait(barrier, n_own - 2)
        tell(barrier, 0, 0)

    @pl.when(sub != 0)
    def _():
        pl.semaphore_wait(barrier, n_own - 1 + sub)

    @pl.when((own == 0) & (sub != 0))
    def _():
        tell(barrier, 0, 0)

    @pl.when(late)
    def _():
        pl.semaphore_wait(barrier, n_own - 1 + n_sub - 1)

    def tell_column(s, carry):
        @pl.when(early & (s > sub))
        def _():
            tell(barrier, own, s)

        @pl.when((own == 1) & (sub == 0) & (s > 0))
        def _():
            tell(barrier, 0, s)

        @pl.when((s < sub) & (own * n_sub + s != 0))
        def _():
            tell(in_sem.at[sub], own, s)

        return carry

    lax.fori_loop(0, n_sub, tell_column, 0)

    def tell_late(i, carry):
        @pl.when(late)
        def _():
            tell(late_sem, i // n_sub, lax.rem(i, n_sub))

        return carry

    lax.fori_loop(1, n, tell_late, 0)

    def send_rows(o, s):
        pltpu.make_async_remote_copy(
            sbuf.at[o * n_sub + s], got_rows.at[me], row_send, row_recv,
            device_id={"owners": o, "sub": s}, device_id_type=MESH,
        ).start()

    def send_meta(o, s):
        pltpu.make_async_remote_copy(
            smeta.at[o * n_sub + s], got_meta.at[me], meta_send, meta_recv,
            device_id={"owners": o, "sub": s}, device_id_type=MESH,
        ).start()

    def peers(act, first, last, which):
        def one(step, carry):
            shift = lax.rem(step * 77, n)
            o = turned(own, shift // n_sub, n_own)
            s = lax.rem(sub + shift, n_sub)

            @pl.when(which(s) & (o * n_sub + s != 0))
            def _():
                act(o, s)

            return carry

        lax.fori_loop(first, last, one, 0)

    peers(send_rows, 1, hold, lambda s: late | (s <= sub))
    own_rows = pltpu.make_async_copy(sbuf.at[me], got_rows.at[me], own_sem.at[0])
    own_rows.start()

    loads[4].wait()
    emb_f = emb[...].astype(F32)
    row_square = jnp.sum(emb_f * emb_f, axis=1, keepdims=True)
    inv_row = lax.rsqrt(jnp.transpose(jnp.broadcast_to(row_square, (rows, 128)))[:1] + 1e-6)
    table_f = table[...].astype(F32)
    inv_class = lax.rsqrt(jnp.sum(table_f * table_f, axis=1, keepdims=True) + 1e-6)
    cosine = dot(table[...], emb[...], ((1,), (1,))) * inv_class
    given = jnp.sum(jnp.where(matches, cosine, 0.0), axis=0, keepdims=True)
    rival = jnp.max(jnp.where(matches, -1e30, cosine), axis=0, keepdims=True)
    margin = (20.0 * ((given - rival) * inv_row)).astype(BF).astype(F32)
    by_rank = jnp.where(rank == iota((8, rows), 0), margin, 0.0).astype(BF)
    scores = dot(named_bf, by_rank, ((1,), (1,)))
    scores = jnp.concatenate([scores, jnp.zeros((n, 120), F32)], axis=1)
    meta = jnp.stack([jnp.broadcast_to(counts, (n, n)), scores], axis=1)
    smeta[...] = meta.astype(BF)

    own_meta = pltpu.make_async_copy(smeta.at[me], got_meta.at[me], own_sem.at[1])
    own_meta.start()

    for first, last in ((1, MIDDLE), (MIDDLE, n_sub)):
        for s in range(first, last):

            @pl.when(early & (s > sub))
            def _(s=s):
                pl.semaphore_wait(in_sem.at[s], 1)

        @pl.when(early & (sub < last - 1))
        def _(first=first, last=last):
            peers(send_rows, 1, hold, lambda s: (s > sub) & (s >= first) & (s < last))

    @pl.when(early)
    def _():
        pl.semaphore_wait(late_sem, 1)

    turn = hold + lax.rem(me, n - hold)

    def held(step, carry):
        @pl.when(early & (step == turn))
        def _():
            send_rows(0, 0)

        shift = lax.rem(step * 77, n)
        o = turned(own, shift // n_sub, n_own)
        s = lax.rem(sub + shift, n_sub)

        @pl.when(o * n_sub + s != 0)
        def _():
            send_rows(o, s)

        return carry

    lax.fori_loop(hold, n, held, 0)
    peers(send_meta, 1, n, lambda s: s >= 0)

    @pl.when(early)
    def _():
        send_meta(0, 0)

    part = pl.ds(0, n - 1)
    pltpu.make_async_copy(sbuf.at[part], got_rows.at[part], row_send).wait()
    pltpu.make_async_copy(smeta.at[part], got_meta.at[part], meta_send).wait()
    own_rows.wait()
    own_meta.wait()
    pltpu.make_async_copy(sbuf.at[part], got_rows.at[part], row_recv).wait()
    pltpu.make_async_copy(smeta.at[part], got_meta.at[part], meta_recv).wait()


def finish(
    n_own, n_sub, cap,
    got_rows, got_meta,
    rows_out, score_out, pos_out, total_out,
    tidy, out_sem,
):
    n = n_own * n_sub
    me = lax.axis_index("owners") * n_sub + lax.axis_index("sub")
    slots = n * cap
    depth = got_rows.shape[-1]
    stores = []
    for g in range(n_own):
        span = pl.ds(g * n_sub * cap, n_sub * cap)
        tidy[span, :] = got_rows[pl.ds(g * n_sub, n_sub)].reshape(n_sub * cap, depth)
        stores.append(pltpu.make_async_copy(tidy.at[span], rows_out.at[span], out_sem.at[g]))
        stores[-1].start()
    got = got_meta[...].astype(F32)
    got_counts, got_scores = got[:, 0, :], got[:, 1, :]
    source = iota((n, slots), 1) // cap
    step_in = lax.rem(iota((1, slots), 1), cap)
    spread = as_bf(iota((n, slots), 0) == source)
    before = as_bf(iota((n, slots), 0) < source)
    counts_bf = got_counts.astype(BF)
    mine = iota((n, slots), 0) == me
    filled = jnp.sum(
        jnp.where(mine, dot(counts_bf, spread, ((0,), (0,))), 0.0), axis=0, keepdims=True
    )
    base = jnp.sum(
        jnp.where(mine, dot(counts_bf, before, ((0,), (0,))), 0.0), axis=0, keepdims=True
    )
    pos_out[...] = jnp.where(
        step_in < filled.astype(jnp.int32), base.astype(jnp.int32) + step_in, -1
    ).reshape(slots)
    spread_scores = dot(got_scores[:, :8].astype(BF), spread, ((0,), (0,)))
    score_out[...] = (
        jnp.sum(
            jnp.where(iota((8, slots), 0) == step_in, spread_scores, 0.0), axis=0, keepdims=True
        )
        .astype(BF)
        .reshape(slots)
    )
    total_out[...] = jnp.sum(got_counts, axis=0, keepdims=True).astype(jnp.int32).reshape(n)
    for store in stores:
        store.wait()


def on_device(n_own, n_sub, embeddings, class_table, nearest, keep_class, destination):
    rows, depth = embeddings.shape
    classes = class_table.shape[0]
    n = n_own * n_sub
    cap = 3 * rows // (2 * n)
    slots = n * cap
    vmem = pl.BlockSpec(memory_space=pltpu.VMEM)
    hbm = pl.BlockSpec(memory_space=pl.ANY)
    got_rows, got_meta = pl.pallas_call(
        functools.partial(exchange, n_own, n_sub, cap),
        out_shape=(
            pltpu.VMEM((n, cap // 2, 2, depth), BF),
            pltpu.VMEM((n, 2, 128), BF),
        ),
        in_specs=[hbm] * 5,
        out_specs=(vmem, vmem),
        scratch_shapes=[
            pltpu.VMEM((rows, depth), BF),
            pltpu.VMEM((classes, depth), BF),
            pltpu.VMEM((1, rows), jnp.int32),
            pltpu.VMEM((1, classes), jnp.int32),
            pltpu.VMEM((1, rows), jnp.int32),
            pltpu.VMEM((n, cap // 2, 2, depth), BF),
            pltpu.VMEM((n, 2, 128), BF),
            pltpu.SemaphoreType.DMA((5,)),
            pltpu.SemaphoreType.DMA((2,)),
            pltpu.SemaphoreType.DMA,
            pltpu.SemaphoreType.DMA,
            pltpu.SemaphoreType.DMA,
            pltpu.SemaphoreType.DMA,
            pltpu.SemaphoreType.REGULAR((n_sub,)),
            pltpu.SemaphoreType.REGULAR,
        ],
        compiler_params=pltpu.CompilerParams(collective_id=0, has_side_effects=True),
    )(
        embeddings,
        class_table,
        nearest.reshape(1, rows),
        keep_class.reshape(1, classes),
        destination.reshape(1, rows),
    )
    return pl.pallas_call(
        functools.partial(finish, n_own, n_sub, cap),
        out_shape=(
            jax.ShapeDtypeStruct((slots, depth), BF),
            jax.ShapeDtypeStruct((slots,), BF),
            jax.ShapeDtypeStruct((slots,), jnp.int32),
            jax.ShapeDtypeStruct((n,), jnp.int32),
        ),
        in_specs=[vmem, vmem],
        out_specs=(hbm, vmem, vmem, vmem),
        scratch_shapes=[
            pltpu.VMEM((slots, depth), BF),
            pltpu.SemaphoreType.DMA((n_own,)),
        ],
    )(
        pltpu.with_memory_space_constraint(got_rows, pltpu.VMEM),
        pltpu.with_memory_space_constraint(got_meta, pltpu.VMEM),
    )


def solution(mesh):
    spec = P(ROWS_AXES)
    return jax.shard_map(
        functools.partial(on_device, mesh.shape["owners"], mesh.shape["sub"]),
        mesh=mesh,
        in_specs=(P(ROWS_AXES, None), P(), spec, P(), P(ROWS_AXES, None)),
        out_specs=(P(ROWS_AXES, None), spec, spec, P("groups")),
        check_vma=False,
    )
```

```python
import functools

import jax
import jax.numpy as jnp
from jax import lax
from jax.experimental import pallas as pl
from jax.experimental.pallas import tpu as pltpu
from jax.sharding import PartitionSpec as P

MESH = pl.DeviceIdType.MESH
BF = jnp.bfloat16
F32 = jnp.float32
ROWS_AXES = ("groups", "owners", "sub")


def iota(shape, dim):
    return lax.broadcasted_iota(jnp.int32, shape, dim)


def as_bf(mask):
    return jnp.where(mask, 1.0, 0.0).astype(BF)


def dot(a, b, dims):
    return lax.dot_general(a, b, (dims, ((), ())), preferred_element_type=F32)


def turned(own, step, n_own):
    chip = lax.rem(own // 2 + step // 2, n_own // 2)
    return chip * 2 + lax.rem(own + step, 2)


def exchange(
    n_own, n_sub, cap,
    emb_hbm, table_hbm, near_hbm, keep_hbm, dest_hbm,
    tidy, got_meta,
    emb, table, near, keep, dest, sbuf, got_rows, smeta,
    load_sem, own_sem, row_send, row_recv, meta_send, meta_recv, in_sem, late_sem,
):
    own, sub = lax.axis_index("owners"), lax.axis_index("sub")
    n = n_own * n_sub
    me = own * n_sub + sub
    rows, depth = emb.shape
    classes = table.shape[0]

    barrier = pltpu.get_barrier_semaphore()
    has_late = lax.axis_index("groups") == 0
    late = has_late & (me == 0)

    def apart(o, s):
        return has_late & (o == 0) & (s == 0)
    hold = n * 5 // 8
    early = jnp.logical_not(late)

    def tell(sem, o, s):
        pl.semaphore_signal(
            sem, inc=1, device_id={"owners": o, "sub": s}, device_id_type=MESH
        )

    loads = [
        pltpu.make_async_copy(src, dst, load_sem.at[i])
        for i, (src, dst) in enumerate(
            (
                (near_hbm, near),
                (keep_hbm, keep),
                (dest_hbm, dest),
                (emb_hbm, emb),
                (table_hbm, table),
            )
        )
    ]
    for load in loads:
        load.start()

    def greet_row(step, carry):
        o = turned(own, step, n_own)

        @pl.when(early & jnp.logical_not(apart(o, sub)))
        def _():
            tell(barrier, o, sub)

        return carry

    lax.fori_loop(1, n_own, greet_row, 0)

    loads[0].wait()
    loads[1].wait()
    loads[2].wait()
    near_v = near[...]
    matches = near_v == iota((classes, rows), 0)
    kept = dot(keep[...].astype(F32).astype(BF), as_bf(matches), ((1,), (0,)))
    named = (dest[...] == iota((n, rows), 0)) & (kept > 0.5)
    named_bf = as_bf(named)
    earlier = as_bf(iota((rows, rows), 0) < iota((rows, rows), 1))
    running = dot(named_bf, earlier, ((1,), (0,)))
    rank = jnp.sum(jnp.where(named, running, 0.0), axis=0, keepdims=True).astype(jnp.int32)
    slot = jnp.where(kept > 0.5, dest[...] * cap + rank, -1)
    place = as_bf(slot == iota((n * cap, rows), 0))
    counts = dot(jnp.ones((8, rows), BF), named_bf, ((1,), (1,)))[:1]

    loads[3].wait()
    packed = dot(place, emb[...], ((1,), (0,))).astype(BF)
    sbuf[...] = packed.reshape(n, cap // 2, 2, depth)

    @pl.when(early & (sub == 0) & has_late)
    def _():
        pl.semaphore_wait(barrier, n_own - 2)
        tell(barrier, 0, 0)

    @pl.when((sub == 0) & jnp.logical_not(has_late))
    def _():
        pl.semaphore_wait(barrier, n_own - 1)

    @pl.when(sub != 0)
    def _():
        pl.semaphore_wait(barrier, n_own - 1 + sub)

    @pl.when(has_late & (own == 0) & (sub != 0))
    def _():
        tell(barrier, 0, 0)

    @pl.when(late)
    def _():
        pl.semaphore_wait(barrier, n_own - 1 + n_sub - 1)

    def tell_column(s, carry):
        @pl.when(early & (s > sub))
        def _():
            tell(barrier, own, s)

        @pl.when(has_late & (own == 1) & (sub == 0) & (s > 0))
        def _():
            tell(barrier, 0, s)

        @pl.when((s < sub) & jnp.logical_not(apart(own, s)))
        def _():
            tell(in_sem.at[sub], own, s)

        return carry

    lax.fori_loop(0, n_sub, tell_column, 0)

    def tell_late(i, carry):
        @pl.when(late)
        def _():
            tell(late_sem, i // n_sub, lax.rem(i, n_sub))

        return carry

    lax.fori_loop(1, n, tell_late, 0)

    def send_rows(o, s):
        pltpu.make_async_remote_copy(
            sbuf.at[o * n_sub + s], got_rows.at[me], row_send, row_recv.at[own],
            device_id={"owners": o, "sub": s}, device_id_type=MESH,
        ).start()

    def send_meta(o, s):
        pltpu.make_async_remote_copy(
            smeta.at[o * n_sub + s], got_meta.at[me], meta_send, meta_recv,
            device_id={"owners": o, "sub": s}, device_id_type=MESH,
        ).start()

    def peers(act, first, last, which):
        def one(step, carry):
            shift = lax.rem(step * 77, n)
            o = turned(own, shift // n_sub, n_own)
            s = lax.rem(sub + shift, n_sub)

            @pl.when(which(s) & jnp.logical_not(apart(o, s)))
            def _():
                act(o, s)

            return carry

        lax.fori_loop(first, last, one, 0)

    peers(send_rows, 1, hold, lambda s: late | (s <= sub))
    pltpu.make_async_copy(sbuf.at[me], got_rows.at[me], row_recv.at[own]).start()

    loads[4].wait()
    emb_f = emb[...].astype(F32)
    row_square = jnp.sum(emb_f * emb_f, axis=1, keepdims=True)
    inv_row = lax.rsqrt(jnp.transpose(jnp.broadcast_to(row_square, (rows, 128)))[:1] + 1e-6)
    table_f = table[...].astype(F32)
    inv_class = lax.rsqrt(jnp.sum(table_f * table_f, axis=1, keepdims=True) + 1e-6)
    cosine = dot(table[...], emb[...], ((1,), (1,))) * inv_class
    given = jnp.sum(jnp.where(matches, cosine, 0.0), axis=0, keepdims=True)
    rival = jnp.max(jnp.where(matches, -1e30, cosine), axis=0, keepdims=True)
    margin = (20.0 * ((given - rival) * inv_row)).astype(BF).astype(F32)
    by_rank = jnp.where(rank == iota((8, rows), 0), margin, 0.0).astype(BF)
    scores = dot(named_bf, by_rank, ((1,), (1,)))
    scores = jnp.concatenate([scores, jnp.zeros((n, 120), F32)], axis=1)
    meta = jnp.stack([jnp.broadcast_to(counts, (n, n)), scores], axis=1)
    smeta[...] = meta.astype(BF)

    own_meta = pltpu.make_async_copy(smeta.at[me], got_meta.at[me], own_sem)
    own_meta.start()

    for s in range(1, n_sub):

        @pl.when(early & (s > sub))
        def _(s=s):
            pl.semaphore_wait(in_sem.at[s], 1)

    @pl.when(early & (sub < n_sub - 1))
    def _():
        peers(send_rows, 1, hold, lambda s: s > sub)

    @pl.when(early & has_late)
    def _():
        pl.semaphore_wait(late_sem, 1)

    turn = hold + lax.rem(me, n - hold)

    def held(step, carry):
        @pl.when(early & has_late & (step == turn))
        def _():
            send_rows(0, 0)

        shift = lax.rem(step * 77, n)
        o = turned(own, shift // n_sub, n_own)
        s = lax.rem(sub + shift, n_sub)

        @pl.when(jnp.logical_not(apart(o, s)))
        def _():
            send_rows(o, s)

        return carry

    lax.fori_loop(hold, n, held, 0)
    peers(send_meta, 1, n, lambda s: s >= 0)

    @pl.when(early & has_late)
    def _():
        send_meta(0, 0)

    part = pl.ds(0, n - 1)
    pltpu.make_async_copy(sbuf.at[part], got_rows.at[part], row_send).wait()
    pltpu.make_async_copy(smeta.at[part], got_meta.at[part], meta_send).wait()
    own_meta.wait()
    for g in (*range(1, n_own), 0):
        block = pl.ds(g * n_sub, n_sub)
        pltpu.make_async_copy(sbuf.at[block], got_rows.at[block], row_recv.at[g]).wait()
        tidy[pl.ds(g * n_sub * cap, n_sub * cap), :] = got_rows[block].reshape(
            n_sub * cap, depth
        )
    pltpu.make_async_copy(smeta.at[part], got_meta.at[part], meta_recv).wait()


def finish(
    n_own, n_sub, cap,
    tidy, got_meta,
    rows_out, score_out, pos_out, total_out,
    out_sem,
):
    n = n_own * n_sub
    me = lax.axis_index("owners") * n_sub + lax.axis_index("sub")
    slots = n * cap
    store = pltpu.make_async_copy(tidy, rows_out, out_sem)
    store.start()
    got = got_meta[...].astype(F32)
    got_counts, got_scores = got[:, 0, :], got[:, 1, :]
    source = iota((n, slots), 1) // cap
    step_in = lax.rem(iota((1, slots), 1), cap)
    spread = as_bf(iota((n, slots), 0) == source)
    before = as_bf(iota((n, slots), 0) < source)
    counts_bf = got_counts.astype(BF)
    mine = iota((n, slots), 0) == me
    filled = jnp.sum(
        jnp.where(mine, dot(counts_bf, spread, ((0,), (0,))), 0.0), axis=0, keepdims=True
    )
    base = jnp.sum(
        jnp.where(mine, dot(counts_bf, before, ((0,), (0,))), 0.0), axis=0, keepdims=True
    )
    pos_out[...] = jnp.where(
        step_in < filled.astype(jnp.int32), base.astype(jnp.int32) + step_in, -1
    ).reshape(slots)
    spread_scores = dot(got_scores[:, :8].astype(BF), spread, ((0,), (0,)))
    score_out[...] = (
        jnp.sum(
            jnp.where(iota((8, slots), 0) == step_in, spread_scores, 0.0), axis=0, keepdims=True
        )
        .astype(BF)
        .reshape(slots)
    )
    total_out[...] = jnp.sum(got_counts, axis=0, keepdims=True).astype(jnp.int32).reshape(n)
    store.wait()


def on_device(n_own, n_sub, embeddings, class_table, nearest, keep_class, destination):
    rows, depth = embeddings.shape
    classes = class_table.shape[0]
    n = n_own * n_sub
    cap = 3 * rows // (2 * n)
    slots = n * cap
    vmem = pl.BlockSpec(memory_space=pltpu.VMEM)
    hbm = pl.BlockSpec(memory_space=pl.ANY)
    tidy, got_meta = pl.pallas_call(
        functools.partial(exchange, n_own, n_sub, cap),
        out_shape=(
            pltpu.VMEM((slots, depth), BF),
            pltpu.VMEM((n, 2, 128), BF),
        ),
        in_specs=[hbm] * 5,
        out_specs=(vmem, vmem),
        scratch_shapes=[
            pltpu.VMEM((rows, depth), BF),
            pltpu.VMEM((classes, depth), BF),
            pltpu.VMEM((1, rows), jnp.int32),
            pltpu.VMEM((1, classes), jnp.int32),
            pltpu.VMEM((1, rows), jnp.int32),
            pltpu.VMEM((n, cap // 2, 2, depth), BF),
            pltpu.VMEM((n, cap // 2, 2, depth), BF),
            pltpu.VMEM((n, 2, 128), BF),
            pltpu.SemaphoreType.DMA((5,)),
            pltpu.SemaphoreType.DMA,
            pltpu.SemaphoreType.DMA,
            pltpu.SemaphoreType.DMA((n_own,)),
            pltpu.SemaphoreType.DMA,
            pltpu.SemaphoreType.DMA,
            pltpu.SemaphoreType.REGULAR((n_sub,)),
            pltpu.SemaphoreType.REGULAR,
        ],
        compiler_params=pltpu.CompilerParams(collective_id=0, has_side_effects=True),
    )(
        embeddings,
        class_table,
        nearest.reshape(1, rows),
        keep_class.reshape(1, classes),
        destination.reshape(1, rows),
    )
    return pl.pallas_call(
        functools.partial(finish, n_own, n_sub, cap),
        out_shape=(
            jax.ShapeDtypeStruct((slots, depth), BF),
            jax.ShapeDtypeStruct((slots,), BF),
            jax.ShapeDtypeStruct((slots,), jnp.int32),
            jax.ShapeDtypeStruct((n,), jnp.int32),
        ),
        in_specs=[vmem, vmem],
        out_specs=(hbm, vmem, vmem, vmem),
        scratch_shapes=[
            pltpu.SemaphoreType.DMA,
        ],
    )(
        pltpu.with_memory_space_constraint(tidy, pltpu.VMEM),
        pltpu.with_memory_space_constraint(got_meta, pltpu.VMEM),
    )


def solution(mesh):
    spec = P(ROWS_AXES)
    return jax.shard_map(
        functools.partial(on_device, mesh.shape["owners"], mesh.shape["sub"]),
        mesh=mesh,
        in_specs=(P(ROWS_AXES, None), P(), spec, P(), P(ROWS_AXES, None)),
        out_specs=(P(ROWS_AXES, None), spec, spec, P("groups")),
        check_vma=False,
    )
```

```python
import functools

import jax
import jax.numpy as jnp
from jax import lax
from jax.experimental import pallas as pl
from jax.experimental.pallas import tpu as pltpu
from jax.sharding import PartitionSpec as P

MESH = pl.DeviceIdType.MESH
BF = jnp.bfloat16
F32 = jnp.float32
ROWS_AXES = ("groups", "owners", "sub")


def iota(shape, dim):
    return lax.broadcasted_iota(jnp.int32, shape, dim)


def as_bf(mask):
    return jnp.where(mask, 1.0, 0.0).astype(BF)


def dot(a, b, dims):
    return lax.dot_general(a, b, (dims, ((), ())), preferred_element_type=F32)


def turned(own, step, n_own):
    chip = lax.rem(own // 2 + step // 2, n_own // 2)
    return chip * 2 + lax.rem(own + step, 2)


def exchange(
    n_own, n_sub, cap,
    emb_hbm, table_hbm, near_hbm, keep_hbm, dest_hbm,
    tidy, got_meta,
    emb, table, near, keep, dest, sbuf, got_rows, smeta,
    load_sem, own_sem, row_send, row_recv, meta_send, meta_recv, in_sem, late_sem,
):
    own, sub = lax.axis_index("owners"), lax.axis_index("sub")
    n = n_own * n_sub
    me = own * n_sub + sub
    rows, depth = emb.shape
    classes = table.shape[0]

    barrier = pltpu.get_barrier_semaphore()
    has_late = lax.axis_index("groups") == 0
    late = has_late & (me == 0)

    def apart(o, s):
        return has_late & (o == 0) & (s == 0)
    hold = n * 19 // 32
    early = jnp.logical_not(late)

    def tell(sem, o, s):
        pl.semaphore_signal(
            sem, inc=1, device_id={"owners": o, "sub": s}, device_id_type=MESH
        )

    loads = [
        pltpu.make_async_copy(src, dst, load_sem.at[i])
        for i, (src, dst) in enumerate(
            (
                (near_hbm, near),
                (keep_hbm, keep),
                (dest_hbm, dest),
                (emb_hbm, emb),
                (table_hbm, table),
            )
        )
    ]
    for load in loads:
        load.start()

    def greet_row(step, carry):
        o = turned(own, step, n_own)

        @pl.when(early & jnp.logical_not(apart(o, sub)))
        def _():
            tell(barrier, o, sub)

        return carry

    lax.fori_loop(1, n_own, greet_row, 0)

    @pl.when(late)
    def _():
        pl.semaphore_wait(barrier, n_own - 1 + n_sub - 1)

    def tell_late(i, carry):
        @pl.when(late)
        def _():
            tell(late_sem, i // n_sub, lax.rem(i, n_sub))

        return carry

    lax.fori_loop(1, n, tell_late, 0)

    loads[0].wait()
    loads[1].wait()
    loads[2].wait()
    near_v = near[...]
    matches = near_v == iota((classes, rows), 0)
    kept = dot(keep[...].astype(F32).astype(BF), as_bf(matches), ((1,), (0,)))
    named = (dest[...] == iota((n, rows), 0)) & (kept > 0.5)
    named_bf = as_bf(named)
    earlier = as_bf(iota((rows, rows), 0) < iota((rows, rows), 1))
    running = dot(named_bf, earlier, ((1,), (0,)))
    rank = jnp.sum(jnp.where(named, running, 0.0), axis=0, keepdims=True).astype(jnp.int32)
    slot = jnp.where(kept > 0.5, dest[...] * cap + rank, -1)
    place = as_bf(slot == iota((n * cap, rows), 0))
    counts = dot(jnp.ones((8, rows), BF), named_bf, ((1,), (1,)))[:1]

    loads[3].wait()
    packed = dot(place, emb[...], ((1,), (0,))).astype(BF)
    sbuf[...] = packed.reshape(n, cap // 2, 2, depth)

    @pl.when(early & (sub == 0) & has_late)
    def _():
        pl.semaphore_wait(barrier, n_own - 2)
        tell(barrier, 0, 0)

    @pl.when((sub == 0) & jnp.logical_not(has_late))
    def _():
        pl.semaphore_wait(barrier, n_own - 1)

    @pl.when(sub != 0)
    def _():
        pl.semaphore_wait(barrier, n_own - 1 + sub)

    @pl.when(has_late & (own == 0) & (sub != 0))
    def _():
        tell(barrier, 0, 0)

    def tell_column(s, carry):
        @pl.when(early & (s > sub))
        def _():
            tell(barrier, own, s)

        @pl.when(has_late & (own == 1) & (sub == 0) & (s > 0))
        def _():
            tell(barrier, 0, s)

        @pl.when((s < sub) & jnp.logical_not(apart(own, s)))
        def _():
            tell(in_sem.at[sub], own, s)

        return carry

    lax.fori_loop(0, n_sub, tell_column, 0)

    def send_rows(o, s):
        pltpu.make_async_remote_copy(
            sbuf.at[o * n_sub + s], got_rows.at[me], row_send, row_recv.at[own],
            device_id={"owners": o, "sub": s}, device_id_type=MESH,
        ).start()

    def send_meta(o, s):
        pltpu.make_async_remote_copy(
            smeta.at[o * n_sub + s], got_meta.at[me], meta_send, meta_recv,
            device_id={"owners": o, "sub": s}, device_id_type=MESH,
        ).start()

    def peers(act, first, last, which):
        def one(step, carry):
            shift = lax.rem(step * 77, n)
            o = turned(own, shift // n_sub, n_own)
            s = lax.rem(sub + shift, n_sub)

            @pl.when(which(s) & jnp.logical_not(apart(o, s)))
            def _():
                act(o, s)

            return carry

        lax.fori_loop(first, last, one, 0)

    peers(send_rows, 1, hold, lambda s: late | (s <= sub))
    pltpu.make_async_copy(sbuf.at[me], got_rows.at[me], row_recv.at[own]).start()

    loads[4].wait()
    emb_f = emb[...].astype(F32)
    row_square = jnp.sum(emb_f * emb_f, axis=1, keepdims=True)
    inv_row = lax.rsqrt(jnp.transpose(jnp.broadcast_to(row_square, (rows, 128)))[:1] + 1e-6)
    table_f = table[...].astype(F32)
    inv_class = lax.rsqrt(jnp.sum(table_f * table_f, axis=1, keepdims=True) + 1e-6)
    cosine = dot(table[...], emb[...], ((1,), (1,))) * inv_class
    given = jnp.sum(jnp.where(matches, cosine, 0.0), axis=0, keepdims=True)
    rival = jnp.max(jnp.where(matches, -1e30, cosine), axis=0, keepdims=True)
    margin = (20.0 * ((given - rival) * inv_row)).astype(BF).astype(F32)
    by_rank = jnp.where(rank == iota((8, rows), 0), margin, 0.0).astype(BF)
    scores = dot(named_bf, by_rank, ((1,), (1,)))
    scores = jnp.concatenate([scores, jnp.zeros((n, 120), F32)], axis=1)
    meta = jnp.stack([jnp.broadcast_to(counts, (n, n)), scores], axis=1)
    smeta[...] = meta.astype(BF)

    own_meta = pltpu.make_async_copy(smeta.at[me], got_meta.at[me], own_sem)
    own_meta.start()

    for s in range(1, n_sub):

        @pl.when(early & (s > sub))
        def _(s=s):
            pl.semaphore_wait(in_sem.at[s], 1)

    @pl.when(early & (sub < n_sub - 1))
    def _():
        peers(send_rows, 1, hold, lambda s: s > sub)

    @pl.when(early & has_late)
    def _():
        pl.semaphore_wait(late_sem, 1)

    turn = hold + lax.rem(me, n - hold)

    def held(step, carry):
        @pl.when(early & has_late & (step == turn))
        def _():
            send_rows(0, 0)

        shift = lax.rem(step * 77, n)
        o = turned(own, shift // n_sub, n_own)
        s = lax.rem(sub + shift, n_sub)

        @pl.when(jnp.logical_not(apart(o, s)))
        def _():
            send_rows(o, s)

        return carry

    lax.fori_loop(hold, n, held, 0)
    peers(send_meta, 1, n, lambda s: s >= 0)

    @pl.when(early & has_late)
    def _():
        send_meta(0, 0)

    part = pl.ds(0, n - 1)
    pltpu.make_async_copy(sbuf.at[part], got_rows.at[part], row_send).wait()
    pltpu.make_async_copy(smeta.at[part], got_meta.at[part], meta_send).wait()
    own_meta.wait()
    for g in (*range(1, n_own), 0):
        block = pl.ds(g * n_sub, n_sub)
        pltpu.make_async_copy(sbuf.at[block], got_rows.at[block], row_recv.at[g]).wait()
        tidy[pl.ds(g * n_sub * cap, n_sub * cap), :] = got_rows[block].reshape(
            n_sub * cap, depth
        )
    pltpu.make_async_copy(smeta.at[part], got_meta.at[part], meta_recv).wait()


def finish(
    n_own, n_sub, cap,
    tidy, got_meta,
    rows_out, score_out, pos_out, total_out,
    out_sem,
):
    n = n_own * n_sub
    me = lax.axis_index("owners") * n_sub + lax.axis_index("sub")
    slots = n * cap
    store = pltpu.make_async_copy(tidy, rows_out, out_sem)
    store.start()
    got = got_meta[...].astype(F32)
    got_counts, got_scores = got[:, 0, :], got[:, 1, :]
    source = iota((n, slots), 1) // cap
    step_in = lax.rem(iota((1, slots), 1), cap)
    spread = as_bf(iota((n, slots), 0) == source)
    before = as_bf(iota((n, slots), 0) < source)
    counts_bf = got_counts.astype(BF)
    mine = iota((n, slots), 0) == me
    filled = jnp.sum(
        jnp.where(mine, dot(counts_bf, spread, ((0,), (0,))), 0.0), axis=0, keepdims=True
    )
    base = jnp.sum(
        jnp.where(mine, dot(counts_bf, before, ((0,), (0,))), 0.0), axis=0, keepdims=True
    )
    pos_out[...] = jnp.where(
        step_in < filled.astype(jnp.int32), base.astype(jnp.int32) + step_in, -1
    ).reshape(slots)
    spread_scores = dot(got_scores[:, :8].astype(BF), spread, ((0,), (0,)))
    score_out[...] = (
        jnp.sum(
            jnp.where(iota((8, slots), 0) == step_in, spread_scores, 0.0), axis=0, keepdims=True
        )
        .astype(BF)
        .reshape(slots)
    )
    total_out[...] = jnp.sum(got_counts, axis=0, keepdims=True).astype(jnp.int32).reshape(n)
    store.wait()


def on_device(n_own, n_sub, embeddings, class_table, nearest, keep_class, destination):
    rows, depth = embeddings.shape
    classes = class_table.shape[0]
    n = n_own * n_sub
    cap = 3 * rows // (2 * n)
    slots = n * cap
    vmem = pl.BlockSpec(memory_space=pltpu.VMEM)
    hbm = pl.BlockSpec(memory_space=pl.ANY)
    tidy, got_meta = pl.pallas_call(
        functools.partial(exchange, n_own, n_sub, cap),
        out_shape=(
            pltpu.VMEM((slots, depth), BF),
            pltpu.VMEM((n, 2, 128), BF),
        ),
        in_specs=[hbm] * 5,
        out_specs=(vmem, vmem),
        scratch_shapes=[
            pltpu.VMEM((rows, depth), BF),
            pltpu.VMEM((classes, depth), BF),
            pltpu.VMEM((1, rows), jnp.int32),
            pltpu.VMEM((1, classes), jnp.int32),
            pltpu.VMEM((1, rows), jnp.int32),
            pltpu.VMEM((n, cap // 2, 2, depth), BF),
            pltpu.VMEM((n, cap // 2, 2, depth), BF),
            pltpu.VMEM((n, 2, 128), BF),
            pltpu.SemaphoreType.DMA((5,)),
            pltpu.SemaphoreType.DMA,
            pltpu.SemaphoreType.DMA,
            pltpu.SemaphoreType.DMA((n_own,)),
            pltpu.SemaphoreType.DMA,
            pltpu.SemaphoreType.DMA,
            pltpu.SemaphoreType.REGULAR((n_sub,)),
            pltpu.SemaphoreType.REGULAR,
        ],
        compiler_params=pltpu.CompilerParams(collective_id=0, has_side_effects=True),
    )(
        embeddings,
        class_table,
        nearest.reshape(1, rows),
        keep_class.reshape(1, classes),
        destination.reshape(1, rows),
    )
    return pl.pallas_call(
        functools.partial(finish, n_own, n_sub, cap),
        out_shape=(
            jax.ShapeDtypeStruct((slots, depth), BF),
            jax.ShapeDtypeStruct((slots,), BF),
            jax.ShapeDtypeStruct((slots,), jnp.int32),
            jax.ShapeDtypeStruct((n,), jnp.int32),
        ),
        in_specs=[vmem, vmem],
        out_specs=(hbm, vmem, vmem, vmem),
        scratch_shapes=[
            pltpu.SemaphoreType.DMA,
        ],
    )(
        pltpu.with_memory_space_constraint(tidy, pltpu.VMEM),
        pltpu.with_memory_space_constraint(got_meta, pltpu.VMEM),
    )


def solution(mesh):
    spec = P(ROWS_AXES)
    return jax.shard_map(
        functools.partial(on_device, mesh.shape["owners"], mesh.shape["sub"]),
        mesh=mesh,
        in_specs=(P(ROWS_AXES, None), P(), spec, P(), P(ROWS_AXES, None)),
        out_specs=(P(ROWS_AXES, None), spec, spec, P("groups")),
        check_vma=False,
    )
```
